256 devices in a mesh: cfg: 2 (over z), ta: 128 (over y, x, core).
Axes of the slice: x: 8, y: 8, z: 2, core: 2. Of those that a mesh axis runs over, the one named last changes fastest.
The devices are a block of a 8x8x16 slice.
Arguments:
- fine_source: bfloat16 [256, 128, 2, 2, 24, 128], P('cfg', 'ta'), parts along dimension 0, may hold values from -24 to 24
- projectors: bfloat16 [256, 128, 2304], P(('cfg', 'ta')), parts along dimension 0, may hold values from -0.21875 to 0.21875
- stencil_links: bfloat16 [256, 8, 48, 864], P(('cfg', 'ta')), parts along dimension 0, may hold values from -0.21875 to 0.21875
- quark_mass: float32 [2], P('cfg'), parts along dimension 0, may hold values from 1.5 to 3
Outputs:
- solution: float32 [256, 8, 96, 128], P(('cfg', 'ta')), parts along dimension 0
- residual: float32 [256, 8, 96, 128], P(('cfg', 'ta')), parts along dimension 0
The draws below stay inside these ranges and needn't reach their ends.
There are 2 independent parts, one for each index of `cfg`. The reference program is written for one: setup_inputs(seed, part) draws one part's arguments, and reference() takes and returns one part's arrays. A program takes and returns all parts, laid end to end along the dimension named above; each array names one. Nothing has to cross between parts.
All inputs are finite; a program needn't handle non-finite values.
Results may differ from the reference program's by a relative error of at most 0.012.
The reference program's roundings to bfloat16 on the way count: a program that leaves them out, or rounds other values in their place, can miss the bound.
Values may be sent and summed in bfloat16 or wider, within the bound.
A program may use at most 128 MiB of HBM per device.

```python
import math
import jax
import jax.numpy as jnp
from jax import lax

NV = 24
LX = 4
LY = 2
LZ = 8
YX = 16
RHS = 128
ITERS = 3
CC = 48
LT = 16
PLANES = 128
XY = 8
COLS = 128
FK = 24


def draw_fine_source(key, part):
    shape_full = (PLANES, COLS, 2, 2, FK, RHS)
    key_base = jax.random.fold_in(key, 11)
    first_key = jax.random.fold_in(key_base, 0)
    third_key = jax.random.fold_in(key_base, 2)
    slices = (jnp.arange(PLANES) // LZ).astype(jnp.float32) / max(LT - 1, 1)
    values = jax.random.truncated_normal(first_key, -4.0, 4.0, shape_full)
    scales = jnp.exp(jax.random.uniform(third_key, (PLANES, COLS, 1, 1, 1, 1), minval=math.log(0.25), maxval=math.log(2.5)))
    time_ramp = jnp.exp(math.log(3.0) * slices - 0.5 * math.log(3.0))
    return (values * scales * time_ramp.reshape(PLANES, 1, 1, 1, 1, 1)).astype(jnp.bfloat16)


def steps_of(rng, extent, cuts, low, high):
    loudness, own = 1.0, jax.random.fold_in(rng, 6)
    for axis_at, parts in cuts:
        heights = jnp.exp(jax.random.uniform(jax.random.fold_in(own, axis_at), (parts,), jnp.float32, low / len(cuts), high / len(cuts)))
        loudness = loudness * jnp.repeat(heights, extent[axis_at] // parts).reshape([-1 if axis == axis_at else 1 for axis in range(len(extent))])
    return loudness


def normal_values(own_key, extent, spread, most, pieces=(), held_as=jnp.bfloat16):
    gain = steps_of(own_key, extent, pieces, -0.22, 0.18) if pieces else 1.0
    array = jax.random.normal(own_key, extent, jnp.float32) * spread * gain
    return jnp.minimum(jnp.maximum(array, -most), most).astype(held_as)


def setup_inputs(seed: int = 0, part: int = 0) -> dict:
    key_of = jax.random.split(jax.random.key(seed), 5)
    part_splits = jax.random.split(jax.random.fold_in(key_of[4], part), 5)
    return {
        "fine_source": draw_fine_source(jax.random.fold_in(jax.random.fold_in(key_of[4], part), 71), part),
        "projectors": normal_values(part_splits[1], (PLANES, COLS, 4 * NV * FK), (2 * YX * FK) ** -0.5, 0.21875, ((0, 128),)),
        "stencil_links": normal_values(part_splits[2], (PLANES, XY, CC, 18 * CC), (18 * CC) ** -0.5, 0.21875, ((0, 128),)),
        "quark_mass": jnp.clip(jax.random.uniform(part_splits[3], (1,), jnp.float32, 1.5, 3.0), 1.5, 3.0),
    }


roll_table = ((0, 0), (3, -1), (3, 1), (2, -1), (2, 1), (1, -1), (1, 1), (0, -1), (0, 1))

def restrict_plane(operands):
    fine_plane, proj_plane = operands
    fine_plane = fine_plane.astype(jnp.float32).reshape(XY, YX, 2, 2, FK, RHS)
    proj_plane = proj_plane.astype(jnp.float32).reshape(XY, YX, 2, NV, 2, FK)
    proj_re = proj_plane[:, :, :, :, 0, :]
    proj_im = proj_plane[:, :, :, :, 1, :]
    fine_re = fine_plane[:, :, 0]
    fine_im = fine_plane[:, :, 1]
    highest = lax.Precision.HIGHEST
    result_re = jnp.einsum('sohvk,sohkr->shvr', proj_re, fine_re, precision=highest) + jnp.einsum('sohvk,sohkr->shvr', proj_im, fine_im, precision=highest)
    result_im = jnp.einsum('sohvk,sohkr->shvr', proj_re, fine_im, precision=highest) - jnp.einsum('sohvk,sohkr->shvr', proj_im, fine_re, precision=highest)
    return jnp.stack([result_re, result_im], axis=1).reshape(XY, 2 * CC, RHS)

def apply_operator(vector, stencil_links, quark_mass):
    highest = lax.Precision.HIGHEST
    rounded = lax.optimization_barrier(vector.astype(jnp.bfloat16)).astype(jnp.float32)
    lattice = rounded.reshape(LT, LZ, LY, LX, 2 * CC, RHS)
    link_view = stencil_links.reshape(PLANES, XY, CC, 9, 2, CC)
    total_re = quark_mass[0] * rounded[:, :, :CC]
    total_im = quark_mass[0] * rounded[:, :, CC:]
    for direction in range(9):
        axis_number, offset = roll_table[direction]
        if direction == 0:
            neighbour = lattice
        else:
            neighbour = jnp.roll(lattice, offset, axis=axis_number)
        neighbour = neighbour.reshape(PLANES, XY, 2 * CC, RHS)
        near_re = neighbour[:, :, :CC]
        near_im = neighbour[:, :, CC:]
        link_re = link_view[:, :, :, direction, 0, :].astype(jnp.float32)
        link_im = link_view[:, :, :, direction, 1, :].astype(jnp.float32)
        total_re = total_re + jnp.einsum('psij,psjr->psir', link_re, near_re, precision=highest) - jnp.einsum('psij,psjr->psir', link_im, near_im, precision=highest)
        total_im = total_im + jnp.einsum('psij,psjr->psir', link_re, near_im, precision=highest) + jnp.einsum('psij,psjr->psir', link_im, near_re, precision=highest)
    return jnp.concatenate([total_re, total_im], axis=2)

def inner_product(left, right):
    left_re = left[:, :, :CC]
    left_im = left[:, :, CC:]
    right_re = right[:, :, :CC]
    right_im = right[:, :, CC:]
    return (lax.optimization_barrier(jnp.sum(left_re * right_re + left_im * right_im, axis=(0, 1, 2))), lax.optimization_barrier(jnp.sum(left_re * right_im - left_im * right_re, axis=(0, 1, 2))))

def scaled(vector, factor_re, factor_im):
    vector_re = vector[..., :CC, :]
    vector_im = vector[..., CC:, :]
    return jnp.concatenate([factor_re * vector_re - factor_im * vector_im, factor_re * vector_im + factor_im * vector_re], axis=-2)

def reference(fine_source, projectors, stencil_links, quark_mass):
    source = lax.map(restrict_plane, (fine_source, projectors))
    solution = jnp.zeros_like(source)
    residual = source
    basis_q = []
    basis_p = []
    for iteration in range(ITERS):
        direction = residual
        mapped = apply_operator(residual, stencil_links, quark_mass)
        coeffs = [inner_product(earlier, mapped) for earlier in basis_q]
        for number in range(iteration):
            mapped = mapped - scaled(basis_q[number], coeffs[number][0], coeffs[number][1])
            direction = direction - scaled(basis_p[number], coeffs[number][0], coeffs[number][1])
        squared = inner_product(mapped, mapped)[0]
        factor = 1.0 / jnp.sqrt(squared + 1e-06)
        unit_q = mapped * factor
        unit_p = direction * factor
        alpha_re, alpha_im = inner_product(unit_q, residual)
        solution = solution + scaled(unit_p, alpha_re, alpha_im)
        residual = residual - scaled(unit_q, alpha_re, alpha_im)
        basis_q.append(unit_q)
        basis_p.append(unit_p)
    return (solution, residual)
```

```python
import functools

import jax
import jax.numpy as jnp
from jax import lax
from jax.experimental import pallas as pl
from jax.experimental.pallas import tpu as pltpu
from jax.sharding import Mesh
from jax.sharding import PartitionSpec as P

YC, XC, CORES = 8, 8, 2
LX = 4
HALF = XC // 2
ITERS = 3
GROUP = ("y", "x", "core")
ALL = ("cfg", "y", "x", "core")
MESH = pl.DeviceIdType.MESH
CHUNKS = 2
F32, BF16 = jnp.float32, jnp.bfloat16


def slot_of(x, core):
    z = 2 * (x % HALF) + core
    return (XC - z) % XC, 1 - x // HALF


def home_of(x, core):
    z = (XC - x) % XC
    return HALF * (1 - core) + z // 2, z % 2


def real_weights(proj_view):
    proj_re = proj_view[..., 0, :]
    proj_im = proj_view[..., 1, :]
    first_row = jnp.stack([proj_re, proj_im], axis=-4)
    second_row = jnp.stack([-proj_im, proj_re], axis=-4)
    return jnp.stack([first_row, second_row], axis=-5)


def solve_kernel(
    mass_ref, source_ref, links_ref, sol_ref, res_ref,
    r_buf, w_buf, halo, q_buf, p_buf, row_send, row_recv, col_send, col_recv, out_send, out_recv,
    src_ss, src_rs, halo_ss, halo_rs, row_ss, row_rs, col_ss, col_rs, out_ss, out_rs,
):
    sites, full, rhs = source_ref.shape
    comps = full // 2
    part = sites // CHUNKS
    g, y, x, core = (lax.axis_index(name) for name in ALL)
    rem, div = lax.rem, lax.div
    z_home = 2 * rem(x, HALF) + core
    to_slot = (g, y, rem(XC - z_home, XC), 1 - div(x, HALF))
    z_slot = rem(XC - x, XC)
    to_home = (g, y, HALF * (1 - core) + div(z_slot, 2), rem(z_slot, 2))
    odd = 1 - core
    upper = (g, y, rem(x + XC - 1, XC), core)
    lower = (g, y, rem(x + 1, XC), core)
    mate = (g, y, x, 1 - core)
    beyond = (g, rem(y + YC - 1 + 2 * odd, YC), x, 1 - core)
    row_peers = [
        (g, y, rem(x + d // 2, XC), rem(core + d % 2, CORES)) for d in range(1, XC * CORES)
    ]
    col_peers = [(g, rem(y + d, YC), x, core) for d in range(1, YC)]

    barrier = pltpu.get_barrier_semaphore()
    everyone = row_peers + col_peers + [beyond]
    for peer in everyone:
        pl.semaphore_signal(barrier, inc=1, device_id=peer, device_id_type=MESH)
    pl.semaphore_wait(barrier, len(everyone))

    def remote(src, dst, send_sem, recv_sem, peer):
        return pltpu.make_async_remote_copy(
            src_ref=src, dst_ref=dst, send_sem=send_sem, recv_sem=recv_sem,
            device_id=peer, device_id_type=MESH,
        )

    def chunk(c):
        return pl.ds(c * part, part)

    pending = []

    def start(copy):
        copy.start()
        pending.append(copy)

    for c in range(CHUNKS):
        start(remote(source_ref.at[chunk(c)], r_buf.at[0, chunk(c)], src_ss.at[c], src_rs.at[c], to_slot))

    def send_halo(k, c):
        src = w_buf.at[k, chunk(c)]
        for kind, peer in ((1, upper), (0, lower), (3 - odd, mate), (2 + odd, beyond)):
            place = {0: 0, 1: 1}.get(kind, 2) if isinstance(kind, int) else (2 if peer is mate else 3)
            start(
                remote(
                    src, halo.at[k, kind, chunk(c)], halo_ss.at[k, place, c], halo_rs.at[k, kind, c], peer
                )
            )

    def wait_halo(k):
        for kind in range(4):
            for c in range(CHUNKS):
                remote(
                    w_buf.at[k, chunk(c)], halo.at[k, kind, chunk(c)],
                    halo_ss.at[k, 0, c], halo_rs.at[k, kind, c], mate,
                ).wait_recv()

    def split(array):
        return array[:comps], array[comps:]

    def gains(vectors):
        rows = []
        for vector in vectors:
            re, im = split(vector)
            rows.append(
                jnp.concatenate(
                    [jnp.concatenate([re, im], axis=1), jnp.concatenate([-im, re], axis=1)], axis=0
                )
            )
        return jnp.concatenate(rows, axis=0)

    def folded(array):
        return jnp.sum(array.reshape(comps // 8, 8, rhs), axis=0)

    mass = mass_ref[0]
    span = 4 * full

    def matvec(k):
        local = []
        for s in range(sites):
            line, col = s // LX, s % LX
            near = [
                s,
                line * LX + (col + 1) % LX,
                line * LX + (col + LX - 1) % LX,
                (s + LX) % sites,
            ]
            local.append(
                jnp.dot(
                    links_ref[s, :, 0:span], gains([w_buf[k, n] for n in near]),
                    preferred_element_type=F32,
                )
            )
        wait_halo(k)
        sums = None
        for s in range(sites):
            second = gains(
                [w_buf[k, (s + sites - LX) % sites]] + [halo[k, kind, s] for kind in range(3)]
            )
            third = gains([halo[k, 3, s]])
            out = local[s]
            out = out + jnp.dot(links_ref[s, :, span:2 * span], second, preferred_element_type=F32)
            out = out + jnp.dot(links_ref[s, :, 2 * span:], third, preferred_element_type=F32)
            own_re, own_im = split(w_buf[k, s].astype(F32))
            q_re = out[:, :rhs] + mass * own_re
            q_im = out[:, rhs:] + mass * own_im
            q_buf[k, s, 0:comps] = q_re
            q_buf[k, s, comps:full] = q_im
            r_re, r_im = split(r_buf[k, s])
            terms = [
                folded(q_re * q_re + q_im * q_im),
                folded(q_re * r_re + q_im * r_im),
                folded(q_re * r_im - q_im * r_re),
            ]
            for j in range(k):
                e_re, e_im = split(q_buf[j, s])
                terms += [
                    folded(e_re * q_re + e_im * q_im),
                    folded(e_re * q_im - e_im * q_re),
                    folded(e_re * r_re + e_im * r_im),
                    folded(e_re * r_im - e_im * r_re),
                ]
            sums = terms if sums is None else [a + b for a, b in zip(sums, terms)]
        return [jnp.sum(one, axis=0, keepdims=True) for one in sums]

    def all_reduce(k, sums):
        count = len(sums)
        rows = pl.ds(0, count)
        for i, one in enumerate(sums):
            row_send[k, i:i + 1, :] = one
        for d, peer in enumerate(row_peers):
            start(
                remote(row_send.at[k, rows], row_recv.at[k, d, rows], row_ss.at[k, d], row_rs.at[k, d], peer)
            )
        total = row_send[k, 0:count]
        for d in range(len(row_peers)):
            remote(
                row_send.at[k, rows], row_recv.at[k, d, rows], row_ss.at[k, d], row_rs.at[k, d], mate
            ).wait_recv()
            total = total + row_recv[k, d, 0:count]
        col_send[k, 0:count] = total
        for d, peer in enumerate(col_peers):
            start(
                remote(col_send.at[k, rows], col_recv.at[k, d, rows], col_ss.at[k, d], col_rs.at[k, d], peer)
            )
        for d in range(len(col_peers)):
            remote(
                col_send.at[k, rows], col_recv.at[k, d, rows], col_ss.at[k, d], col_rs.at[k, d], mate
            ).wait_recv()
            total = total + col_recv[k, d, 0:count]
        return [total[i:i + 1] for i in range(count)]

    def minus(value, coefs, basis, s):
        re, im = split(value)
        for j, (c_re, c_im) in enumerate(coefs):
            e_re, e_im = split(basis[j, s])
            re = re - (c_re * e_re - c_im * e_im)
            im = im - (c_re * e_im + c_im * e_re)
        return re, im

    for c in range(CHUNKS):
        remote(source_ref.at[chunk(c)], r_buf.at[0, chunk(c)], src_ss.at[c], src_rs.at[c], mate).wait_recv()
        for s in range(c * part, (c + 1) * part):
            w_buf[0, s] = r_buf[0, s].astype(BF16)
        send_halo(0, c)

    gram = {}
    alphas = []
    factors = []
    for k in range(ITERS):
        totals = all_reduce(k, matvec(k))
        squared, a_re, a_im = totals[:3]
        coefs = []
        for j in range(k):
            c_re, c_im, b_re, b_im = totals[3 + 4 * j:7 + 4 * j]
            coefs.append((c_re, c_im))
            a_re = a_re - (c_re * b_re + c_im * b_im)
            a_im = a_im - (c_re * b_im - c_im * b_re)
        for j, (c_re, c_im) in enumerate(coefs):
            squared = squared - (2.0 - gram[j, j][0]) * (c_re * c_re + c_im * c_im)
        for i in range(k):
            for j in range(i + 1, k):
                (u_re, u_im), (v_re, v_im) = coefs[i], coefs[j]
                m_re = u_re * v_re + u_im * v_im
                m_im = u_re * v_im - u_im * v_re
                n_re, n_im = gram[i, j]
                squared = squared + 2.0 * (m_re * n_re - m_im * n_im)
        squared = jnp.maximum(squared, 0.0)
        factor = 1.0 / jnp.sqrt(squared + 1e-06)
        if k + 1 < ITERS:
            gram[k, k] = (squared * factor * factor, None)
            for j, (c_re, c_im) in enumerate(coefs):
                lack_re = (1.0 - gram[j, j][0]) * c_re
                lack_im = (1.0 - gram[j, j][0]) * c_im
                gram[j, k] = (factor * lack_re, factor * lack_im)
        a_re, a_im = a_re * factor, a_im * factor
        alphas.append((a_re, a_im))
        factors.append(factor)
        last = k + 1 == ITERS
        for c in range(CHUNKS):
            for s in range(c * part, (c + 1) * part):
                q_re, q_im = minus(q_buf[k, s], coefs, q_buf, s)
                q_re, q_im = q_re * factor, q_im * factor
                r_re, r_im = split(r_buf[k, s])
                r_re = r_re - (a_re * q_re - a_im * q_im)
                r_im = r_im - (a_re * q_im + a_im * q_re)
                if last:
                    out_send[1, s, 0:comps] = r_re.astype(BF16)
                    out_send[1, s, comps:full] = r_im.astype(BF16)
                else:
                    q_buf[k, s, 0:comps] = q_re
                    q_buf[k, s, comps:full] = q_im
                    r_buf[k + 1, s, 0:comps] = r_re
                    r_buf[k + 1, s, comps:full] = r_im
                    w_buf[k + 1, s, 0:comps] = r_re.astype(BF16)
                    w_buf[k + 1, s, comps:full] = r_im.astype(BF16)
            if last:
                start(
                    remote(
                        out_send.at[1, chunk(c)], out_recv.at[1, chunk(c)], out_ss.at[1, c], out_rs.at[1, c],
                        to_home,
                    )
                )
            else:
                send_halo(k + 1, c)
        for c in range(CHUNKS):
            for s in range(c * part, (c + 1) * part):
                p_re, p_im = minus(r_buf[k, s], coefs, p_buf, s)
                p_re, p_im = p_re * factor, p_im * factor
                if last:
                    s_re = a_re * p_re - a_im * p_im
                    s_im = a_re * p_im + a_im * p_re
                    for j in range(k):
                        e_re, e_im = split(p_buf[j, s])
                        b_re, b_im = alphas[j]
                        s_re = s_re + (b_re * e_re - b_im * e_im)
                        s_im = s_im + (b_re * e_im + b_im * e_re)
                    out_send[0, s, 0:comps] = s_re.astype(BF16)
                    out_send[0, s, comps:full] = s_im.astype(BF16)
                else:
                    p_buf[k, s, 0:comps] = p_re
                    p_buf[k, s, comps:full] = p_im
            if last:
                start(
                    remote(
                        out_send.at[0, chunk(c)], out_recv.at[0, chunk(c)], out_ss.at[0, c], out_rs.at[0, c],
                        to_home,
                    )
                )
    for which, target in ((1, res_ref), (0, sol_ref)):
        for c in range(CHUNKS):
            remote(
                out_send.at[which, chunk(c)], out_recv.at[which, chunk(c)],
                out_ss.at[which, c], out_rs.at[which, c], mate,
            ).wait_recv()
            for s in range(c * part, (c + 1) * part):
                target[s] = out_recv[which, s].astype(F32)
    for copy in pending:
        copy.wait_send()


def solve(source, links, mass):
    sites, full, rhs = source.shape
    vector = (sites, full, rhs)
    most = 3 + 4 * (ITERS - 1)
    rows = -(-most // 8) * 8
    peers_x, peers_y = XC * CORES - 1, YC - 1
    dma = pltpu.SemaphoreType.DMA
    vmem = pl.BlockSpec(memory_space=pltpu.VMEM)
    return pl.pallas_call(
        solve_kernel,
        out_shape=(jax.ShapeDtypeStruct(vector, F32), jax.ShapeDtypeStruct(vector, F32)),
        in_specs=[pl.BlockSpec(memory_space=pltpu.SMEM), vmem, vmem],
        out_specs=(vmem, vmem),
        scratch_shapes=[
            pltpu.VMEM((ITERS,) + vector, F32),
            pltpu.VMEM((ITERS,) + vector, BF16),
            pltpu.VMEM((ITERS, 4) + vector, BF16),
            pltpu.VMEM((ITERS,) + vector, F32),
            pltpu.VMEM((ITERS - 1,) + vector, F32),
            pltpu.VMEM((ITERS, rows, rhs), F32),
            pltpu.VMEM((ITERS, peers_x, rows, rhs), F32),
            pltpu.VMEM((ITERS, rows, rhs), F32),
            pltpu.VMEM((ITERS, peers_y, rows, rhs), F32),
            pltpu.VMEM((2,) + vector, BF16),
            pltpu.VMEM((2,) + vector, BF16),
            dma((CHUNKS,)), dma((CHUNKS,)),
            dma((ITERS, 4, CHUNKS)), dma((ITERS, 4, CHUNKS)),
            dma((ITERS, peers_x)), dma((ITERS, peers_x)),
            dma((ITERS, peers_y)), dma((ITERS, peers_y)),
            dma((2, CHUNKS)), dma((2, CHUNKS)),
        ],
        compiler_params=pltpu.CompilerParams(
            collective_id=0, has_side_effects=True, vmem_limit_bytes=48 * 1024 * 1024
        ),
        name="gcr_solve",
    )(mass, source, links)


def shards(fine_source, projectors, stencil_links, quark_mass):
    comp_count = stencil_links.shape[2]
    null_count = comp_count // 2
    site_count = stencil_links.shape[1]
    column_count = projectors.shape[1]
    block_count = column_count // site_count
    fine_count = fine_source.shape[4]
    rhs_count = fine_source.shape[5]
    moves = [
        (x * CORES + c, slot_of(x, c)[0] * CORES + slot_of(x, c)[1])
        for x in range(XC) for c in range(CORES)
    ]
    links = lax.ppermute(stencil_links[0], ("x", "core"), moves)
    regrouped = lax.all_to_all(fine_source, GROUP, split_axis=0, concat_axis=1, tiled=True)
    fine_local = regrouped.reshape(site_count, block_count, 2, 2, fine_count, rhs_count)
    weights = real_weights(
        projectors.reshape(site_count, block_count, 2, null_count, 2, fine_count)
    )
    source = jnp.einsum(
        "sodchvk,sochkr->sdhvr", weights, fine_local, preferred_element_type=jnp.float32
    )
    source = source.reshape(site_count, 2 * comp_count, rhs_count)
    solution, residual = solve(source, links, quark_mass)
    return solution[None], residual[None]


def solution(mesh):
    finer = Mesh(mesh.devices.reshape(mesh.shape["cfg"], YC, XC, CORES), ALL)
    placed = (
        P("cfg", GROUP, None, None, None, None),
        P(ALL, None, None),
        P(ALL, None, None, None),
        P("cfg"),
    )
    return jax.shard_map(
        shards,
        mesh=finer,
        in_specs=placed,
        out_specs=(P(ALL, None, None, None), P(ALL, None, None, None)),
        check_vma=False,
    )
```

```python
import jax
import jax.numpy as jnp
from jax import lax
from jax.experimental import pallas as pl
from jax.experimental.pallas import tpu as pltpu
from jax.sharding import Mesh
from jax.sharding import PartitionSpec as P

YC, XC, CORES = 8, 8, 2
LX = 4
HALF = XC // 2
ITERS = 3
GROUP = ("y", "x", "core")
ALL = ("cfg", "y", "x", "core")
MESH = pl.DeviceIdType.MESH
CHUNKS = 2
FK = 24
F32, BF16 = jnp.float32, jnp.bfloat16


def solve_kernel(
    mass_ref, fine_ref, proj_ref, far_links_ref, sol_ref, res_ref,
    fine_buf, raw, wide, spread, blocks, pbuf, chain_send, chain_recv, total_buf, links_ref,
    r_buf, w_buf, halo, q_buf, p_buf, row_send, row_recv, col_send, col_recv, out_send, out_recv,
    links_ss, links_rs, fine_ls, fine_ss, fine_rs, raw_ls, raw_ss, raw_rs, blk_ss, blk_rs,
    chain_ss, chain_rs, src_ss, src_rs,
    halo_ss, halo_rs, row_ss, row_rs, col_ss, col_rs, out_ss, out_rs,
):
    sites, full, rhs = sol_ref.shape
    comps = full // 2
    part = sites // CHUNKS
    g, y, x, core = (lax.axis_index(name) for name in ALL)
    rem, div = lax.rem, lax.div
    z_home = 2 * rem(x, HALF) + core
    to_slot = (g, y, rem(XC - z_home, XC), 1 - div(x, HALF))
    z_slot = rem(XC - x, XC)
    to_home = (g, y, HALF * (1 - core) + div(z_slot, 2), rem(z_slot, 2))
    odd = 1 - core
    upper = (g, y, rem(x + XC - 1, XC), core)
    lower = (g, y, rem(x + 1, XC), core)
    mate = (g, y, x, 1 - core)
    beyond = (g, rem(y + YC - 1 + 2 * odd, YC), x, 1 - core)
    row_peers = [
        (g, y, rem(x + d // 2, XC), rem(core + d % 2, CORES)) for d in range(1, XC * CORES)
    ]
    col_peers = [(g, rem(y + d, YC), x, core) for d in range(1, YC)]

    barrier = pltpu.get_barrier_semaphore()
    everyone = row_peers + col_peers + [beyond]
    for peer in everyone:
        pl.semaphore_signal(barrier, inc=1, device_id=peer, device_id_type=MESH)
    pl.semaphore_wait(barrier, len(everyone))

    def remote(src, dst, send_sem, recv_sem, peer):
        return pltpu.make_async_remote_copy(
            src_ref=src, dst_ref=dst, send_sem=send_sem, recv_sem=recv_sem,
            device_id=peer, device_id_type=MESH,
        )

    def chunk(c):
        return pl.ds(c * part, part)

    pending = []

    def start(copy):
        copy.start()
        pending.append(copy)

    start(remote(far_links_ref, links_ref, links_ss, links_rs, to_slot))
    for dy, peer in enumerate(col_peers):
        rows = pl.ds(pl.multiple_of(rem(y + 1 + dy, YC) * 16, 16), 16)
        start(remote(proj_ref.at[rows], raw.at[y], raw_ss.at[dy], raw_rs.at[dy], peer))
    own_raw = pltpu.make_async_copy(proj_ref.at[pl.ds(pl.multiple_of(y * 16, 16), 16)], raw.at[y], raw_ls)
    own_raw.start()
    own_fine = []
    for reim in range(2):
        for h in range(2):
            i = 2 * reim + h
            rows = pl.ds(pl.multiple_of(reim * comps + core * FK, FK), FK)
            start(
                remote(
                    fine_ref.at[:, core, :, reim, h], fine_buf.at[:, :, h, rows], fine_ss.at[i], fine_rs.at[i], mate
                )
            )
            copy = pltpu.make_async_copy(
                fine_ref.at[:, 1 - core, :, reim, h], fine_buf.at[:, :, h, rows], fine_ls.at[i]
            )
            copy.start()
            own_fine.append(copy)

    own_raw.wait()
    for dy in range(YC - 1):
        remote(proj_ref.at[pl.ds(0, 16)], raw.at[y], raw_ss.at[dy], raw_rs.at[dy], mate).wait_recv()
    tiles = wide.shape[0]
    for t in range(tiles):
        for yp in range(YC):
            wide[t, 16 * yp:16 * yp + 16] = raw[yp, :, 128 * t:128 * (t + 1)].astype(F32)
    lanes = lax.broadcasted_iota(jnp.int32, (XC * YC, 128), 1)

    def spread_group(group, carry):
        for v in range(8):
            acc = jnp.zeros((XC * YC, 128), F32)
            for c in range(CORES):
                held = {}
                for reim in range(2):
                    first = 2 * FK * v + FK * reim
                    to = 2 * FK * reim + FK * c
                    left = FK
                    while left:
                        tile, off = first // 128, first % 128
                        size = min(left, 128 - off)
                        if tile not in held:
                            held[tile] = wide[3 * group + tile, pl.ds(c, XC * YC, stride=CORES), :]
                        moved = pltpu.roll(held[tile], (to - off) % 128, 1) if to != off else held[tile]
                        acc = jnp.where((lanes >= to) & (lanes < to + size), moved, acc)
                        first, to, left = first + size, to + size, left - size
            spread[pl.ds(8 * group + v, XC * YC, stride=comps), :] = acc
        return carry

    lax.fori_loop(0, comps // 8, spread_group, 0)
    for xc in range(XC):
        for yp in range(YC):
            base = (yp * XC + xc) * comps
            blocks[xc, yp] = spread[base:base + comps].astype(BF16)
    owner = 1 - div(x, HALF)
    home_slot = rem(XC - z_home, XC)
    for i, step in enumerate((4, 3, 5, 2, 6, 1, 7, 0)):
        xc = rem(home_slot + step, XC)
        here = jnp.logical_and(xc == x, owner == core)
        copy = remote(blocks.at[xc], pbuf.at[z_home], blk_ss.at[i], blk_rs.at[z_home], (g, y, xc, owner))

        @pl.when(here)
        def _():
            pbuf[z_home] = blocks[xc]

        @pl.when(jnp.logical_not(here))
        def _():
            copy.start()

    def product(z, yp):
        lhs = pbuf[z, yp]
        outs = []
        for h in range(2):
            left = fine_buf[yp, z, h]
            right = jnp.concatenate([left[comps:], -left[:comps]], axis=0)
            out = jnp.dot(
                lhs[16 * h:16 * h + 32, :full], jnp.concatenate([left, right], axis=1),
                preferred_element_type=F32,
            )
            outs.append(out[8 * h:8 * h + FK])
        return jnp.concatenate([part_[:, :rhs] for part_ in outs] + [part_[:, rhs:] for part_ in outs], axis=0)

    def wait_blocks(z):
        mine = jnp.logical_and(z == z_home, owner == core)

        @pl.when(jnp.logical_not(mine))
        def _():
            remote(blocks.at[0], pbuf.at[z], blk_ss.at[0], blk_rs.at[z], mate).wait_recv()

    for copy in own_fine:
        copy.wait()
    for i in range(4):
        remote(
            fine_ref.at[:, 0, :, 0, 0], fine_buf.at[:, :, 0, pl.ds(0, FK)], fine_ss.at[i], fine_rs.at[i], mate
        ).wait_recv()

    ways = ((1, (g, y, rem(x + 1, XC), core)), (0, (g, y, rem(x + XC - 1, XC), core)))
    steps = (4, 3, 3, 2, 2, 1, 1)
    for m, d in enumerate(steps):
        for way, (plus, peer) in enumerate(ways):
            dest = rem(x + (d if plus else XC - d), XC)
            z = rem(XC - dest, XC)
            if (m == 0 and way == 0) or m in (1, 3, 5):
                wait_blocks(z)
            if m >= 2:
                remote(
                    chain_send.at[way, m - 2], chain_recv.at[way, m - 2],
                    chain_ss.at[way, m - 2], chain_rs.at[way, m - 2], mate,
                ).wait_recv()
            upper_half = (m + 1 - plus) % 2

            def body(i, carry):
                value = product(z, upper_half * 4 + i)
                if m >= 2:
                    value = value + chain_recv[way, m - 2, i]
                chain_send[way, m, i] = value
                return carry

            lax.fori_loop(0, YC // 2, body, 0)
            start(
                remote(
                    chain_send.at[way, m], chain_recv.at[way, m], chain_ss.at[way, m], chain_rs.at[way, m], peer
                )
            )
    z = rem(XC - x, XC)
    wait_blocks(z)
    for way in range(2):
        for m in (5, 6):
            remote(
                chain_send.at[way, m], chain_recv.at[way, m], chain_ss.at[way, m], chain_rs.at[way, m], mate
            ).wait_recv()
    for dy in (4, 3, 5, 2, 6, 1, 7, 0):
        yp = rem(y + dy, YC)
        high, i = div(yp, YC // 2), rem(yp, YC // 2)
        value = product(z, yp) + chain_recv[0, 6 - high, i] + chain_recv[1, 5 + high, i]
        if dy == 0:
            r_buf[0, y] = value
        else:
            total_buf[dy] = value
            start(
                remote(total_buf.at[dy], r_buf.at[0, y], src_ss.at[dy - 1], src_rs.at[dy - 1], (g, yp, x, core))
            )

    def send_halo(k, c):
        src = w_buf.at[k, chunk(c)]
        for kind, peer in ((1, upper), (0, lower), (3 - odd, mate), (2 + odd, beyond)):
            place = {0: 0, 1: 1}.get(kind, 2) if isinstance(kind, int) else (2 if peer is mate else 3)
            start(
                remote(
                    src, halo.at[k, kind, chunk(c)], halo_ss.at[k, place, c], halo_rs.at[k, kind, c], peer
                )
            )

    def wait_halo(k):
        for kind in range(4):
            for c in range(CHUNKS):
                remote(
                    w_buf.at[k, chunk(c)], halo.at[k, kind, chunk(c)],
                    halo_ss.at[k, 0, c], halo_rs.at[k, kind, c], mate,
                ).wait_recv()

    def split(array):
        return array[:comps], array[comps:]

    def gains(vectors):
        rows = []
        for vector in vectors:
            re, im = split(vector)
            rows.append(
                jnp.concatenate(
                    [jnp.concatenate([re, im], axis=1), jnp.concatenate([-im, re], axis=1)], axis=0
                )
            )
        return jnp.concatenate(rows, axis=0)

    def folded(array):
        return jnp.sum(array.reshape(comps // 8, 8, rhs), axis=0)

    mass = mass_ref[0]
    span = 4 * full

    def matvec(k):
        local = []
        for s in range(sites):
            line, col = s // LX, s % LX
            near = [
                s,
                line * LX + (col + 1) % LX,
                line * LX + (col + LX - 1) % LX,
                (s + LX) % sites,
            ]
            local.append(
                jnp.dot(
                    links_ref[s, :, 0:span], gains([w_buf[k, n] for n in near]),
                    preferred_element_type=F32,
                )
            )
        wait_halo(k)
        sums = None
        for s in range(sites):
            second = gains(
                [w_buf[k, (s + sites - LX) % sites]] + [halo[k, kind, s] for kind in range(3)]
            )
            third = gains([halo[k, 3, s]])
            out = local[s]
            out = out + jnp.dot(links_ref[s, :, span:2 * span], second, preferred_element_type=F32)
            out = out + jnp.dot(links_ref[s, :, 2 * span:], third, preferred_element_type=F32)
            own_re, own_im = split(w_buf[k, s].astype(F32))
            q_re = out[:, :rhs] + mass * own_re
            q_im = out[:, rhs:] + mass * own_im
            q_buf[k, s, 0:comps] = q_re
            q_buf[k, s, comps:full] = q_im
            r_re, r_im = split(r_buf[k, s])
            terms = [
                folded(q_re * q_re + q_im * q_im),
                folded(q_re * r_re + q_im * r_im),
                folded(q_re * r_im - q_im * r_re),
            ]
            for j in range(k):
                e_re, e_im = split(q_buf[j, s])
                terms += [
                    folded(e_re * q_re + e_im * q_im),
                    folded(e_re * q_im - e_im * q_re),
                    folded(e_re * r_re + e_im * r_im),
                    folded(e_re * r_im - e_im * r_re),
                ]
            sums = terms if sums is None else [a + b for a, b in zip(sums, terms)]
        return [jnp.sum(one, axis=0, keepdims=True) for one in sums]

    def all_reduce(k, sums):
        count = len(sums)
        rows = pl.ds(0, count)
        for i, one in enumerate(sums):
            row_send[k, i:i + 1, :] = one
        for d, peer in enumerate(row_peers):
            start(
                remote(row_send.at[k, rows], row_recv.at[k, d, rows], row_ss.at[k, d], row_rs.at[k, d], peer)
            )
        total = row_send[k, 0:count]
        for d in range(len(row_peers)):
            remote(
                row_send.at[k, rows], row_recv.at[k, d, rows], row_ss.at[k, d], row_rs.at[k, d], mate
            ).wait_recv()
            total = total + row_recv[k, d, 0:count]
        col_send[k, 0:count] = total
        for d, peer in enumerate(col_peers):
            start(
                remote(col_send.at[k, rows], col_recv.at[k, d, rows], col_ss.at[k, d], col_rs.at[k, d], peer)
            )
        for d in range(len(col_peers)):
            remote(
                col_send.at[k, rows], col_recv.at[k, d, rows], col_ss.at[k, d], col_rs.at[k, d], mate
            ).wait_recv()
            total = total + col_recv[k, d, 0:count]
        return [total[i:i + 1] for i in range(count)]

    def minus(value, coefs, basis, s):
        re, im = split(value)
        for j, (c_re, c_im) in enumerate(coefs):
            e_re, e_im = split(basis[j, s])
            re = re - (c_re * e_re - c_im * e_im)
            im = im - (c_re * e_im + c_im * e_re)
        return re, im

    for dy in range(1, YC):
        remote(
            total_buf.at[dy], r_buf.at[0, rem(y + YC - dy, YC)], src_ss.at[dy - 1], src_rs.at[dy - 1], mate
        ).wait_recv()
    for c in range(CHUNKS):
        for s in range(c * part, (c + 1) * part):
            w_buf[0, s] = r_buf[0, s].astype(BF16)
        send_halo(0, c)
    remote(far_links_ref, links_ref, links_ss, links_rs, mate).wait_recv()

    gram = {}
    alphas = []
    factors = []
    for k in range(ITERS):
        totals = all_reduce(k, matvec(k))
        squared, a_re, a_im = totals[:3]
        coefs = []
        for j in range(k):
            c_re, c_im, b_re, b_im = totals[3 + 4 * j:7 + 4 * j]
            coefs.append((c_re, c_im))
            a_re = a_re - (c_re * b_re + c_im * b_im)
            a_im = a_im - (c_re * b_im - c_im * b_re)
        for j, (c_re, c_im) in enumerate(coefs):
            squared = squared - (2.0 - gram[j, j][0]) * (c_re * c_re + c_im * c_im)
        for i in range(k):
            for j in range(i + 1, k):
                (u_re, u_im), (v_re, v_im) = coefs[i], coefs[j]
                m_re = u_re * v_re + u_im * v_im
                m_im = u_re * v_im - u_im * v_re
                n_re, n_im = gram[i, j]
                squared = squared + 2.0 * (m_re * n_re - m_im * n_im)
        squared = jnp.maximum(squared, 0.0)
        factor = 1.0 / jnp.sqrt(squared + 1e-06)
        if k + 1 < ITERS:
            gram[k, k] = (squared * factor * factor, None)
            for j, (c_re, c_im) in enumerate(coefs):
                lack_re = (1.0 - gram[j, j][0]) * c_re
                lack_im = (1.0 - gram[j, j][0]) * c_im
                gram[j, k] = (factor * lack_re, factor * lack_im)
        a_re, a_im = a_re * factor, a_im * factor
        alphas.append((a_re, a_im))
        factors.append(factor)
        last = k + 1 == ITERS
        for c in range(CHUNKS):
            for s in range(c * part, (c + 1) * part):
                q_re, q_im = minus(q_buf[k, s], coefs, q_buf, s)
                q_re, q_im = q_re * factor, q_im * factor
                r_re, r_im = split(r_buf[k, s])
                r_re = r_re - (a_re * q_re - a_im * q_im)
                r_im = r_im - (a_re * q_im + a_im * q_re)
                if last:
                    out_send[1, s, 0:comps] = r_re.astype(BF16)
                    out_send[1, s, comps:full] = r_im.astype(BF16)
                else:
                    q_buf[k, s, 0:comps] = q_re
                    q_buf[k, s, comps:full] = q_im
                    r_buf[k + 1, s, 0:comps] = r_re
                    r_buf[k + 1, s, comps:full] = r_im
                    w_buf[k + 1, s, 0:comps] = r_re.astype(BF16)
                    w_buf[k + 1, s, comps:full] = r_im.astype(BF16)
            if last:
                start(
                    remote(
                        out_send.at[1, chunk(c)], out_recv.at[1, chunk(c)], out_ss.at[1, c], out_rs.at[1, c],
                        to_home,
                    )
                )
            else:
                send_halo(k + 1, c)
        for c in range(CHUNKS):
            for s in range(c * part, (c + 1) * part):
                p_re, p_im = minus(r_buf[k, s], coefs, p_buf, s)
                p_re, p_im = p_re * factor, p_im * factor
                if last:
                    s_re = a_re * p_re - a_im * p_im
                    s_im = a_re * p_im + a_im * p_re
                    for j in range(k):
                        e_re, e_im = split(p_buf[j, s])
                        b_re, b_im = alphas[j]
                        s_re = s_re + (b_re * e_re - b_im * e_im)
                        s_im = s_im + (b_re * e_im + b_im * e_re)
                    out_send[0, s, 0:comps] = s_re.astype(BF16)
                    out_send[0, s, comps:full] = s_im.astype(BF16)
                else:
                    p_buf[k, s, 0:comps] = p_re
                    p_buf[k, s, comps:full] = p_im
            if last:
                start(
                    remote(
                        out_send.at[0, chunk(c)], out_recv.at[0, chunk(c)], out_ss.at[0, c], out_rs.at[0, c],
                        to_home,
                    )
                )
    for which, target in ((1, res_ref), (0, sol_ref)):
        for c in range(CHUNKS):
            remote(
                out_send.at[which, chunk(c)], out_recv.at[which, chunk(c)],
                out_ss.at[which, c], out_rs.at[which, c], mate,
            ).wait_recv()
            for s in range(c * part, (c + 1) * part):
                target[s] = out_recv[which, s].astype(F32)
    for copy in pending:
        copy.wait_send()
    for i, step in enumerate((4, 3, 5, 2, 6, 1, 7, 0)):
        xc = rem(home_slot + step, XC)

        @pl.when(jnp.logical_not(jnp.logical_and(xc == x, owner == core)))
        def _():
            remote(blocks.at[xc], pbuf.at[z_home], blk_ss.at[i], blk_rs.at[z_home], mate).wait_send()


def shards(fine_source, projectors, stencil_links, quark_mass):
    sites, comps, width = stencil_links.shape[1:]
    rhs = fine_source.shape[-1]
    full = 2 * comps
    columns, row = projectors.shape[1:]
    fine = fine_source.reshape(YC, 2, XC, 2, 2, FK, rhs)
    vector = (sites, full, rhs)
    most = 3 + 4 * (ITERS - 1)
    rows = -(-most // 8) * 8
    peers_x, peers_y = XC * CORES - 1, YC - 1
    dma = pltpu.SemaphoreType.DMA
    vmem = pl.BlockSpec(memory_space=pltpu.VMEM)
    hbm = pl.BlockSpec(memory_space=pltpu.HBM)
    solution, residual = pl.pallas_call(
        solve_kernel,
        out_shape=(jax.ShapeDtypeStruct(vector, F32), jax.ShapeDtypeStruct(vector, F32)),
        in_specs=[pl.BlockSpec(memory_space=pltpu.SMEM), hbm, hbm, hbm],
        out_specs=(vmem, vmem),
        scratch_shapes=[
            pltpu.VMEM((YC, XC, 2, full, rhs), BF16),
            pltpu.VMEM((YC, columns // YC, row), BF16),
            pltpu.VMEM((row // 128, columns, 128), F32),
            pltpu.VMEM((XC * YC * comps, 128), F32),
            pltpu.VMEM((XC, YC, comps, 128), BF16),
            pltpu.VMEM((XC, YC, comps, 128), BF16),
            pltpu.VMEM((2, 7, YC // 2, full, rhs), F32),
            pltpu.VMEM((2, 7, YC // 2, full, rhs), F32),
            pltpu.VMEM((YC, full, rhs), F32),
            pltpu.VMEM((sites, comps, width), BF16),
            pltpu.VMEM((ITERS,) + vector, F32),
            pltpu.VMEM((ITERS,) + vector, BF16),
            pltpu.VMEM((ITERS, 4) + vector, BF16),
            pltpu.VMEM((ITERS,) + vector, F32),
            pltpu.VMEM((ITERS - 1,) + vector, F32),
            pltpu.VMEM((ITERS, rows, rhs), F32),
            pltpu.VMEM((ITERS, peers_x, rows, rhs), F32),
            pltpu.VMEM((ITERS, rows, rhs), F32),
            pltpu.VMEM((ITERS, peers_y, rows, rhs), F32),
            pltpu.VMEM((2,) + vector, BF16),
            pltpu.VMEM((2,) + vector, BF16),
            dma(()), dma(()),
            dma((4,)), dma((4,)), dma((4,)),
            dma(()), dma((peers_y,)), dma((peers_y,)),
            dma((XC,)), dma((XC,)),
            dma((2, 7)), dma((2, 7)),
            dma((peers_y,)), dma((peers_y,)),
            dma((ITERS, 4, CHUNKS)), dma((ITERS, 4, CHUNKS)),
            dma((ITERS, peers_x)), dma((ITERS, peers_x)),
            dma((ITERS, peers_y)), dma((ITERS, peers_y)),
            dma((2, CHUNKS)), dma((2, CHUNKS)),
        ],
        compiler_params=pltpu.CompilerParams(
            collective_id=0, has_side_effects=True, vmem_limit_bytes=56 * 1024 * 1024
        ),
        name="restrict_and_solve",
    )(quark_mass, fine, projectors[0], stencil_links[0])
    return solution[None], residual[None]


def solution(mesh):
    finer = Mesh(mesh.devices.reshape(mesh.shape["cfg"], YC, XC, CORES), ALL)
    placed = (
        P("cfg", GROUP, None, None, None, None),
        P(ALL, None, None),
        P(ALL, None, None, None),
        P("cfg"),
    )
    return jax.shard_map(
        shards,
        mesh=finer,
        in_specs=placed,
        out_specs=(P(ALL, None, None, None), P(ALL, None, None, None)),
        check_vma=False,
    )
```

```python
import jax
import jax.numpy as jnp
from jax import lax
from jax.experimental import pallas as pl
from jax.experimental.pallas import tpu as pltpu
from jax.sharding import Mesh
from jax.sharding import PartitionSpec as P

YC, XC, CORES = 8, 8, 2
LX = 4
HALF = XC // 2
ITERS = 3
GROUP = ("y", "x", "core")
ALL = ("cfg", "y", "x", "core")
MESH = pl.DeviceIdType.MESH
CHUNKS = 2
EARLY = 5
FK = 24
PACKED = 40
ORDER = (
    ((0, 4), (1, 4), (2, 3), (0, 3), (1, 3), (3, 3), (0, 2), (1, 2), (2, 2), (0, 1), (1, 1), (3, 2), (2, 1), (3, 1)),
    ((0, 3), (1, 3), (2, 4), (3, 4), (0, 2), (1, 2), (2, 3), (3, 3), (0, 1), (1, 1), (2, 2), (3, 2), (2, 1), (3, 1)),
)
F32, BF16 = jnp.float32, jnp.bfloat16


def remote(src, dst, send_sem, recv_sem, peer):
    return pltpu.make_async_remote_copy(
        src_ref=src, dst_ref=dst, send_sem=send_sem, recv_sem=recv_sem,
        device_id=peer, device_id_type=MESH,
    )


def places():
    g, y, x, core = (lax.axis_index(name) for name in ALL)
    z_home = 2 * lax.rem(x, HALF) + core
    z_slot = lax.rem(XC - x, XC)
    to_slot = (g, y, lax.rem(XC - z_home, XC), 1 - lax.div(x, HALF))
    to_home = (g, y, HALF * (1 - core) + lax.div(z_slot, 2), lax.rem(z_slot, 2))
    return g, y, x, core, z_home, z_slot, to_slot, to_home


def meet(peers):
    barrier = pltpu.get_barrier_semaphore()
    for peer in peers:
        pl.semaphore_signal(barrier, inc=1, device_id=peer, device_id_type=MESH)


def met(peers):
    pl.semaphore_wait(pltpu.get_barrier_semaphore(), len(peers))


def solve_kernel(
    mass_ref, fine_ref, proj_ref, far_links_ref, out_recv,
    fine_buf, raw, wide, spread, blocks, packed, pbuf, chain_send, chain_recv, total_buf, links_ref,
    r_buf, w_buf, halo, q_buf, w_home, row_send, row_recv, col_send, col_recv, out_send,
    links_ss, links_rs, fine_ls, fine_ss, fine_rs, raw_ls, raw_ss, raw_rs, blk_ss, blk_rs,
    chain_ss, chain_rs, src_ss, src_rs,
    halo_ss, halo_rs, row_ss, row_rs, col_ss, col_rs, home_ss, home_rs, out_ss, out_rs,
):
    sites, full, rhs = out_recv.shape[1:]
    comps = full // 2
    part = sites // CHUNKS
    rem, div = lax.rem, lax.div
    g, y, x, core, z_home, z_slot, to_slot, to_home = places()
    odd = 1 - core
    upper = (g, y, rem(x + XC - 1, XC), core)
    lower = (g, y, rem(x + 1, XC), core)
    mate = (g, y, x, 1 - core)
    beyond = (g, rem(y + YC - 1 + 2 * odd, YC), x, 1 - core)
    row_peers = [
        (g, y, rem(x + d // 2, XC), rem(core + d % 2, CORES)) for d in range(1, XC * CORES)
    ]
    col_peers = [(g, rem(y + d, YC), x, core) for d in range(1, YC)]

    everyone = row_peers + col_peers + [beyond]
    meet(everyone)

    def chunk(c):
        return pl.ds(c * part, part)

    pending = []

    def start(copy):
        copy.start()
        pending.append(copy)

    def send_halo(k, c):
        src = w_buf.at[k, chunk(c)]
        for kind, peer in ((1, upper), (0, lower), (3 - odd, mate), (2 + odd, beyond)):
            place = {0: 0, 1: 1}.get(kind, 2) if isinstance(kind, int) else (2 if peer is mate else 3)
            start(
                remote(
                    src, halo.at[k, kind, chunk(c)], halo_ss.at[k, place, c], halo_rs.at[k, kind, c], peer
                )
            )

    def wait_halo(k):
        for kind in range(4):
            for c in range(CHUNKS):
                remote(
                    w_buf.at[k, chunk(c)], halo.at[k, kind, chunk(c)],
                    halo_ss.at[k, 0, c], halo_rs.at[k, kind, c], mate,
                ).wait_recv()

    def split(array):
        return array[:comps], array[comps:]

    def gains(vectors):
        rows = []
        for vector in vectors:
            re, im = split(vector)
            rows.append(
                jnp.concatenate(
                    [jnp.concatenate([re, im], axis=1), jnp.concatenate([-im, re], axis=1)], axis=0
                )
            )
        return jnp.concatenate(rows, axis=0)

    def folded(array):
        return jnp.sum(array.reshape(comps // 8, 8, rhs), axis=0)

    mass = mass_ref[0]
    span = 4 * full

    def matvec(k):
        local = []
        for s in range(sites):
            line, col = s // LX, s % LX
            near = [
                s,
                line * LX + (col + 1) % LX,
                line * LX + (col + LX - 1) % LX,
                (s + LX) % sites,
            ]
            local.append(
                jnp.dot(
                    links_ref[s, :, 0:span], gains([w_buf[k, n] for n in near]),
                    preferred_element_type=F32,
                )
            )
        wait_halo(k)
        sums = None
        for s in range(sites):
            second = gains(
                [w_buf[k, (s + sites - LX) % sites]] + [halo[k, kind, s] for kind in range(3)]
            )
            third = gains([halo[k, 3, s]])
            out = local[s]
            out = out + jnp.dot(links_ref[s, :, span:2 * span], second, preferred_element_type=F32)
            out = out + jnp.dot(links_ref[s, :, 2 * span:], third, preferred_element_type=F32)
            own_re, own_im = split(w_buf[k, s].astype(F32))
            q_re = out[:, :rhs] + mass * own_re
            q_im = out[:, rhs:] + mass * own_im
            q_buf[k, s, 0:comps] = q_re
            q_buf[k, s, comps:full] = q_im
            r_re, r_im = split(r_buf[k, s])
            terms = [
                folded(q_re * q_re + q_im * q_im),
                folded(q_re * r_re + q_im * r_im),
                folded(q_re * r_im - q_im * r_re),
            ]
            for j in range(k):
                e_re, e_im = split(q_buf[j, s])
                terms += [
                    folded(e_re * q_re + e_im * q_im),
                    folded(e_re * q_im - e_im * q_re),
                    folded(e_re * r_re + e_im * r_im),
                    folded(e_re * r_im - e_im * r_re),
                ]
            sums = terms if sums is None else [a + b for a, b in zip(sums, terms)]
        return [jnp.sum(one, axis=0, keepdims=True) for one in sums]

    def all_reduce(k, sums):
        count = len(sums)
        rows = pl.ds(0, count)
        for i, one in enumerate(sums):
            row_send[k, i:i + 1, :] = one
        for d, peer in enumerate(row_peers):
            start(
                remote(row_send.at[k, rows], row_recv.at[k, d, rows], row_ss.at[k, d], row_rs.at[k, d], peer)
            )
        total = row_send[k, 0:count]
        for d in range(len(row_peers)):
            remote(
                row_send.at[k, rows], row_recv.at[k, d, rows], row_ss.at[k, d], row_rs.at[k, d], mate
            ).wait_recv()
            total = total + row_recv[k, d, 0:count]
        col_send[k, 0:count] = total
        for d, peer in enumerate(col_peers):
            start(
                remote(col_send.at[k, rows], col_recv.at[k, d, rows], col_ss.at[k, d], col_rs.at[k, d], peer)
            )
        start(remote(w_buf.at[k], w_home.at[k], home_ss.at[k], home_rs.at[k], to_home))
        for d in range(len(col_peers)):
            remote(
                col_send.at[k, rows], col_recv.at[k, d, rows], col_ss.at[k, d], col_rs.at[k, d], mate
            ).wait_recv()
            total = total + col_recv[k, d, 0:count]
        return [total[i:i + 1] for i in range(count)]

    def minus(value, coefs, basis, s):
        re, im = split(value)
        for j, (c_re, c_im) in enumerate(coefs):
            e_re, e_im = split(basis[j, s])
            re = re - (c_re * e_re - c_im * e_im)
            im = im - (c_re * e_im + c_im * e_re)
        return re, im

    columns = raw.shape[1]
    columns = raw.shape[1]
    own_raw = pltpu.make_async_copy(
        proj_ref.at[pl.ds(pl.multiple_of(y * columns, columns), columns)], raw.at[y], raw_ls
    )
    own_fine = []
    for reim in range(2):
        for h in range(2):
            i = 2 * reim + h
            rows = pl.ds(pl.multiple_of(reim * comps + core * FK, FK), FK)
            own_fine.append(
                pltpu.make_async_copy(
                    fine_ref.at[:, 1 - core, :, reim, h], fine_buf.at[:, :, h, rows], fine_ls.at[i]
                )
            )
    for copy in [own_raw] + own_fine:
        copy.start()

    def links_copy(c):
        span_ = (pl.ds(0, EARLY), pl.ds(EARLY, sites - EARLY))[c]
        return remote(far_links_ref.at[span_], links_ref.at[span_], links_ss.at[c], links_rs.at[c], to_slot)

    met(everyone)
    for dy, peer in enumerate(col_peers):
        rows = pl.ds(pl.multiple_of(rem(y + 1 + dy, YC) * columns, columns), columns)
        start(remote(proj_ref.at[rows], raw.at[y], raw_ss.at[dy], raw_rs.at[dy], peer))
    start(links_copy(0))
    for reim in range(2):
        for h in range(2):
            i = 2 * reim + h
            rows = pl.ds(pl.multiple_of(reim * comps + core * FK, FK), FK)
            start(
                remote(
                    fine_ref.at[:, core, :, reim, h], fine_buf.at[:, :, h, rows], fine_ss.at[i], fine_rs.at[i], mate
                )
            )

    own_raw.wait()
    for dy in range(YC - 1):
        remote(proj_ref.at[pl.ds(0, columns)], raw.at[y], raw_ss.at[dy], raw_rs.at[dy], mate).wait_recv()
    tiles = wide.shape[0]
    for t in range(tiles):
        for yp in range(YC):
            wide[t, 16 * yp:16 * yp + 16] = raw[yp, :, 128 * t:128 * (t + 1)].astype(F32)
    lanes = lax.broadcasted_iota(jnp.int32, (XC * YC, 128), 1)

    def spread_group(group, carry):
        for v in range(8):
            acc = jnp.zeros((XC * YC, 128), F32)
            for c in range(CORES):
                held = {}
                for reim in range(2):
                    first = 2 * FK * v + FK * reim
                    to = 2 * FK * reim + FK * c
                    left = FK
                    while left:
                        tile, off = first // 128, first % 128
                        size = min(left, 128 - off)
                        if tile not in held:
                            held[tile] = wide[3 * group + tile, pl.ds(c, XC * YC, stride=CORES), :]
                        moved = pltpu.roll(held[tile], (to - off) % 128, 1) if to != off else held[tile]
                        acc = jnp.where((lanes >= to) & (lanes < to + size), moved, acc)
                        first, to, left = first + size, to + size, left - size
            spread[pl.ds(8 * group + v, XC * YC, stride=comps), :] = acc
        return carry

    lax.fori_loop(0, comps // 8, spread_group, 0)
    lane = lax.broadcasted_iota(jnp.int32, (8, 128), 1)
    low_lanes = lane < full
    for xc in range(XC):
        for yp in range(YC):
            base = (yp * XC + xc) * comps
            tail = spread[base + PACKED:base + comps]
            head = [
                jnp.where(low_lanes, spread[base + 8 * j:base + 8 * j + 8], pltpu.roll(tail, full - 32 * j, 1))
                for j in range(3)
            ]
            blocks[xc, yp] = jnp.concatenate(head + [spread[base + 24:base + PACKED]], axis=0).astype(BF16)
    owner = 1 - div(x, HALF)
    home_slot = rem(XC - z_home, XC)
    for i, step in enumerate((4, 3, 5, 2, 6, 1, 7, 0)):
        xc = rem(home_slot + step, XC)
        here = jnp.logical_and(xc == x, owner == core)
        copy = remote(blocks.at[xc], packed.at[z_home], blk_ss.at[i], blk_rs.at[z_home], (g, y, xc, owner))

        @pl.when(here)
        def _():
            packed[z_home] = blocks[xc]

        @pl.when(jnp.logical_not(here))
        def _():
            copy.start()

    def product(z, yp):
        lhs = pbuf[z, yp]
        outs = []
        for h in range(2):
            left = fine_buf[yp, z, h]
            right = jnp.concatenate([left[comps:], -left[:comps]], axis=0)
            out = jnp.dot(
                lhs[16 * h:16 * h + 32, :full], jnp.concatenate([left, right], axis=1),
                preferred_element_type=F32,
            )
            outs.append(out[8 * h:8 * h + FK])
        return jnp.concatenate([part_[:, :rhs] for part_ in outs] + [part_[:, rhs:] for part_ in outs], axis=0)

    def wait_blocks(z):
        mine = jnp.logical_and(z == z_home, owner == core)

        @pl.when(jnp.logical_not(mine))
        def _():
            remote(blocks.at[0], packed.at[z], blk_ss.at[0], blk_rs.at[z], mate).wait_recv()

        def unpack(yp, carry):
            held = packed[z, yp]
            rows = held[0:24].astype(F32)
            moved = [pltpu.roll(rows[8 * j:8 * j + 8], 32 * (j + 1), 1) for j in range(3)]
            tail = jnp.where(lane < 32, moved[0], jnp.where(lane < 64, moved[1], moved[2]))
            pbuf[z, yp] = jnp.concatenate([held.astype(F32), tail], axis=0).astype(BF16)
            return carry

        lax.fori_loop(0, YC, unpack, 0)

    for copy in own_fine:
        copy.wait()
    for i in range(4):
        remote(
            fine_ref.at[:, 0, :, 0, 0], fine_buf.at[:, :, 0, pl.ds(0, FK)], fine_ss.at[i], fine_rs.at[i], mate
        ).wait_recv()

    ways = ((1, (g, y, rem(x + 1, XC), core)), (0, (g, y, rem(x + XC - 1, XC), core)))
    waited = set()

    def received(way, m):
        remote(
            chain_send.at[way, m], chain_recv.at[way, m], chain_ss.at[way, m], chain_rs.at[way, m], mate
        ).wait_recv()

    def finish(quarter):
        z = z_slot
        if 0 not in waited:
            waited.add(0)
            wait_blocks(z)
        last = [ORDER[way].index((quarter, 1)) for way in range(2)]
        for way in range(2):
            received(way, last[way])
        for i in range(2):
            yp = 2 * quarter + i
            total_buf[yp] = product(z, yp) + chain_recv[0, last[0], i] + chain_recv[1, last[1], i]

            @pl.when(y == yp)
            def _():
                r_buf[0, yp] = total_buf[yp]

            @pl.when(y != yp)
            def _():
                remote(total_buf.at[yp], r_buf.at[0, y], src_ss.at[yp], src_rs.at[y], (g, yp, x, core)).start()

    for m in range(len(ORDER[0])):
        for way, (plus, peer) in enumerate(ways):
            quarter, d = ORDER[way][m]
            sign = d if plus else -d
            z = rem(XC - rem(x + XC + sign, XC), XC)
            key = sign % XC
            if key not in waited:
                waited.add(key)
                wait_blocks(z)
            before = (quarter, d + 1)
            source = ORDER[way].index(before) if before in ORDER[way] else None
            if source is not None:
                received(way, source)
            for i in range(2):
                value = product(z, 2 * quarter + i)
                if source is not None:
                    value = value + chain_recv[way, source, i]
                chain_send[way, m, i] = value
            start(
                remote(
                    chain_send.at[way, m], chain_recv.at[way, m], chain_ss.at[way, m], chain_rs.at[way, m], peer
                )
            )
        if m in (11, 12):
            finish(m - 11)
    start(links_copy(1))
    finish(2)
    finish(3)
    for s in range(sites):

        @pl.when(y != s)
        def _():
            remote(total_buf.at[s], r_buf.at[0, s], src_ss.at[s], src_rs.at[s], mate).wait_recv()

    for c in range(CHUNKS):
        for s in range(c * part, (c + 1) * part):
            w_buf[0, s] = r_buf[0, s].astype(BF16)
        send_halo(0, c)
    for c in range(CHUNKS):
        links_copy(c).wait_recv()

    gram = {}
    basis = []
    betas = []
    for k in range(ITERS):
        totals = all_reduce(k, matvec(k))
        squared, a_re, a_im = totals[:3]
        coefs = []
        for j in range(k):
            c_re, c_im, b_re, b_im = totals[3 + 4 * j:7 + 4 * j]
            coefs.append((c_re, c_im))
            a_re = a_re - (c_re * b_re + c_im * b_im)
            a_im = a_im - (c_re * b_im - c_im * b_re)
        for j, (c_re, c_im) in enumerate(coefs):
            squared = squared - (2.0 - gram[j, j][0]) * (c_re * c_re + c_im * c_im)
        for i in range(k):
            for j in range(i + 1, k):
                (u_re, u_im), (v_re, v_im) = coefs[i], coefs[j]
                m_re = u_re * v_re + u_im * v_im
                m_im = u_re * v_im - u_im * v_re
                n_re, n_im = gram[i, j]
                squared = squared + 2.0 * (m_re * n_re - m_im * n_im)
        squared = jnp.maximum(squared, 0.0)
        factor = 1.0 / jnp.sqrt(squared + 1e-06)
        if k + 1 < ITERS:
            gram[k, k] = (squared * factor * factor, None)
            for j, (c_re, c_im) in enumerate(coefs):
                lack_re = (1.0 - gram[j, j][0]) * c_re
                lack_im = (1.0 - gram[j, j][0]) * c_im
                gram[j, k] = (factor * lack_re, factor * lack_im)
        a_re, a_im = a_re * factor, a_im * factor
        last = k + 1 == ITERS
        for c in range(CHUNKS):
            for s in range(c * part, (c + 1) * part):
                q_re, q_im = minus(q_buf[k, s], coefs, q_buf, s)
                q_re, q_im = q_re * factor, q_im * factor
                r_re, r_im = split(r_buf[k, s])
                r_re = r_re - (a_re * q_re - a_im * q_im)
                r_im = r_im - (a_re * q_im + a_im * q_re)
                if last:
                    out_send[s, 0:comps] = r_re.astype(BF16)
                    out_send[s, comps:full] = r_im.astype(BF16)
                else:
                    q_buf[k, s, 0:comps] = q_re
                    q_buf[k, s, comps:full] = q_im
                    r_buf[k + 1, s, 0:comps] = r_re
                    r_buf[k + 1, s, comps:full] = r_im
                    w_buf[k + 1, s, 0:comps] = r_re.astype(BF16)
                    w_buf[k + 1, s, comps:full] = r_im.astype(BF16)
            if last:
                start(
                    remote(out_send.at[chunk(c)], out_recv.at[1, chunk(c)], out_ss.at[c], out_rs.at[c], to_home)
                )
            else:
                send_halo(k + 1, c)
        row = [(0.0, 0.0)] * k + [(factor, 0.0)]
        for j, (c_re, c_im) in enumerate(coefs):
            f_re, f_im = factor * c_re, factor * c_im
            for i in range(j + 1):
                u_re, u_im = basis[j][i]
                row[i] = (row[i][0] - (f_re * u_re - f_im * u_im), row[i][1] - (f_re * u_im + f_im * u_re))
        basis.append(row)
        for i in range(k + 1):
            u_re, u_im = row[i]
            b_re, b_im = betas[i] if i < len(betas) else (0.0, 0.0)
            term = (b_re + a_re * u_re - a_im * u_im, b_im + a_re * u_im + a_im * u_re)
            betas[i:i + 1] = [term]
    for k in range(ITERS):
        remote(w_buf.at[k], w_home.at[k], home_ss.at[k], home_rs.at[k], mate).wait_recv()
    for s in range(sites):
        s_re = s_im = 0.0
        for k in range(ITERS):
            b_re, b_im = betas[k]
            e_re, e_im = split(w_home[k, s].astype(F32))
            s_re = s_re + (b_re * e_re - b_im * e_im)
            s_im = s_im + (b_re * e_im + b_im * e_re)
        out_recv[0, s, 0:comps] = s_re.astype(BF16)
        out_recv[0, s, comps:full] = s_im.astype(BF16)
    for c in range(CHUNKS):
        remote(out_send.at[chunk(c)], out_recv.at[1, chunk(c)], out_ss.at[c], out_rs.at[c], mate).wait_recv()
    for copy in pending:
        copy.wait_send()
    for i, step in enumerate((4, 3, 5, 2, 6, 1, 7, 0)):
        xc = rem(home_slot + step, XC)

        @pl.when(jnp.logical_not(jnp.logical_and(xc == x, owner == core)))
        def _():
            remote(blocks.at[xc], packed.at[z_home], blk_ss.at[i], blk_rs.at[z_home], mate).wait_send()

    for yp in range(YC):

        @pl.when(y != yp)
        def _():
            remote(total_buf.at[yp], r_buf.at[0, yp], src_ss.at[yp], src_rs.at[yp], mate).wait_send()


def shards(fine_source, projectors, stencil_links, quark_mass):
    sites, comps, width = stencil_links.shape[1:]
    rhs = fine_source.shape[-1]
    full = 2 * comps
    columns, row = projectors.shape[1:]
    fine = fine_source.reshape(YC, 2, XC, 2, 2, FK, rhs)
    vector = (sites, full, rhs)
    most = 3 + 4 * (ITERS - 1)
    rows = -(-most // 8) * 8
    peers_x, peers_y = XC * CORES - 1, YC - 1
    dma = pltpu.SemaphoreType.DMA
    vmem = pl.BlockSpec(memory_space=pltpu.VMEM)
    hbm = pl.BlockSpec(memory_space=pltpu.HBM)
    messages = len(ORDER[0])
    result = pl.pallas_call(
        solve_kernel,
        out_shape=jax.ShapeDtypeStruct((2,) + vector, BF16),
        in_specs=[pl.BlockSpec(memory_space=pltpu.SMEM), hbm, hbm, hbm],
        out_specs=vmem,
        scratch_shapes=[
            pltpu.VMEM((YC, XC, 2, full, rhs), BF16),
            pltpu.VMEM((YC, columns // YC, row), BF16),
            pltpu.VMEM((row // 128, columns, 128), F32),
            pltpu.VMEM((XC * YC * comps, 128), F32),
            pltpu.VMEM((XC, YC, PACKED, 128), BF16),
            pltpu.VMEM((XC, YC, PACKED, 128), BF16),
            pltpu.VMEM((XC, YC, comps, 128), BF16),
            pltpu.VMEM((2, messages, 2, full, rhs), F32),
            pltpu.VMEM((2, messages, 2, full, rhs), F32),
            pltpu.VMEM((YC, full, rhs), F32),
            pltpu.VMEM((sites, comps, width), BF16),
            pltpu.VMEM((ITERS,) + vector, F32),
            pltpu.VMEM((ITERS,) + vector, BF16),
            pltpu.VMEM((ITERS, 4) + vector, BF16),
            pltpu.VMEM((ITERS,) + vector, F32),
            pltpu.VMEM((ITERS,) + vector, BF16),
            pltpu.VMEM((ITERS, rows, rhs), F32),
            pltpu.VMEM((ITERS, peers_x, rows, rhs), F32),
            pltpu.VMEM((ITERS, rows, rhs), F32),
            pltpu.VMEM((ITERS, peers_y, rows, rhs), F32),
            pltpu.VMEM(vector, BF16),
            dma((CHUNKS,)), dma((CHUNKS,)), dma((4,)), dma((4,)), dma((4,)),
            dma(()), dma((peers_y,)), dma((peers_y,)),
            dma((XC,)), dma((XC,)),
            dma((2, messages)), dma((2, messages)),
            dma((YC,)), dma((YC,)),
            dma((ITERS, 4, CHUNKS)), dma((ITERS, 4, CHUNKS)),
            dma((ITERS, peers_x)), dma((ITERS, peers_x)),
            dma((ITERS, peers_y)), dma((ITERS, peers_y)),
            dma((ITERS,)), dma((ITERS,)), dma((CHUNKS,)), dma((CHUNKS,)),
        ],
        compiler_params=pltpu.CompilerParams(
            collective_id=0, has_side_effects=True, vmem_limit_bytes=56 * 1024 * 1024
        ),
        name="restrict_and_solve",
    )(quark_mass, fine, projectors[0], stencil_links[0])
    result = result.astype(F32)
    return result[0:1], result[1:2]


def solution(mesh):
    finer = Mesh(mesh.devices.reshape(mesh.shape["cfg"], YC, XC, CORES), ALL)
    placed = (
        P("cfg", GROUP, None, None, None, None),
        P(ALL, None, None),
        P(ALL, None, None, None),
        P("cfg"),
    )
    return jax.shard_map(
        shards,
        mesh=finer,
        in_specs=placed,
        out_specs=(P(ALL, None, None, None), P(ALL, None, None, None)),
        check_vma=False,
    )
```

```python
import jax
import jax.numpy as jnp
from jax import lax
from jax.experimental import pallas as pl
from jax.experimental.pallas import tpu as pltpu
from jax.sharding import Mesh
from jax.sharding import PartitionSpec as P

YC, XC, CORES = 8, 8, 2
LX = 4
HALF = XC // 2
ITERS = 3
GROUP = ("y", "x", "core")
ALL = ("cfg", "y", "x", "core")
MESH = pl.DeviceIdType.MESH
CHUNKS = 2
EARLY = 5
FK = 24
PACKED = 40
ORDER = (
    ((0, 4), (1, 4), (2, 3), (0, 3), (1, 3), (3, 3), (0, 2), (1, 2), (2, 2), (0, 1), (1, 1), (3, 2), (2, 1), (3, 1)),
    ((0, 3), (1, 3), (2, 4), (3, 4), (0, 2), (1, 2), (2, 3), (3, 3), (0, 1), (1, 1), (2, 2), (3, 2), (2, 1), (3, 1)),
)
F32, BF16 = jnp.float32, jnp.bfloat16


def remote(src, dst, send_sem, recv_sem, peer):
    return pltpu.make_async_remote_copy(
        src_ref=src, dst_ref=dst, send_sem=send_sem, recv_sem=recv_sem,
        device_id=peer, device_id_type=MESH,
    )


def places():
    g, y, x, core = (lax.axis_index(name) for name in ALL)
    z_home = 2 * lax.rem(x, HALF) + core
    z_slot = lax.rem(XC - x, XC)
    to_slot = (g, y, lax.rem(XC - z_home, XC), 1 - lax.div(x, HALF))
    to_home = (g, y, HALF * (1 - core) + lax.div(z_slot, 2), lax.rem(z_slot, 2))
    return g, y, x, core, z_home, z_slot, to_slot, to_home


def meet(peers):
    barrier = pltpu.get_barrier_semaphore()
    for peer in peers:
        pl.semaphore_signal(barrier, inc=1, device_id=peer, device_id_type=MESH)


def met(peers):
    pl.semaphore_wait(pltpu.get_barrier_semaphore(), len(peers))


def solve_kernel(
    mass_ref, fine_ref, proj_ref, far_links_ref, out_recv,
    fine_buf, raw, wide, spread, blocks, packed, pbuf, chain_send, chain_recv, total_buf, links_ref,
    r_buf, w_buf, halo, q_buf, w_home, row_send, row_recv, col_send, col_recv, out_send,
    links_ss, links_rs, fine_ls, fine_ss, fine_rs, raw_ls, raw_ss, raw_rs, blk_ss, blk_rs,
    chain_ss, chain_rs, src_ss, src_rs,
    first_ss, first_rs, halo_ss, halo_rs, row_ss, row_rs, col_ss, col_rs, home_ss, home_rs, out_ss, out_rs,
):
    sites, full, rhs = out_recv.shape[1:]
    comps = full // 2
    part = sites // CHUNKS
    rem, div = lax.rem, lax.div
    g, y, x, core, z_home, z_slot, to_slot, to_home = places()
    odd = 1 - core
    upper = (g, y, rem(x + XC - 1, XC), core)
    lower = (g, y, rem(x + 1, XC), core)
    mate = (g, y, x, 1 - core)
    beyond = (g, rem(y + YC - 1 + 2 * odd, YC), x, 1 - core)
    row_peers = [
        (g, y, rem(x + d // 2, XC), rem(core + d % 2, CORES)) for d in range(1, XC * CORES)
    ]
    col_peers = [(g, rem(y + d, YC), x, core) for d in range(1, YC)]

    everyone = row_peers + col_peers + [beyond]
    meet(everyone)

    def chunk(c):
        return pl.ds(c * part, part)

    pending = []

    def start(copy):
        copy.start()
        pending.append(copy)

    neighbours = ((1, upper), (0, lower), (3 - odd, mate), (2 + odd, beyond))

    def send_halo(k, c):
        for place, (kind, peer) in enumerate(neighbours):
            start(
                remote(
                    w_buf.at[k, chunk(c)], halo.at[k, kind, chunk(c)],
                    halo_ss.at[k, place, c], halo_rs.at[k, kind, c], peer,
                )
            )

    def wait_halo(k):
        for kind in range(4):
            if k == 0:
                for s in range(sites):
                    remote(
                        w_buf.at[0, s], halo.at[0, kind, s], first_ss.at[0, s], first_rs.at[kind, s], mate
                    ).wait_recv()
                continue
            for c in range(CHUNKS):
                remote(
                    w_buf.at[k, chunk(c)], halo.at[k, kind, chunk(c)],
                    halo_ss.at[k, 0, c], halo_rs.at[k, kind, c], mate,
                ).wait_recv()

    def split(array):
        return array[:comps], array[comps:]

    def gains(vectors):
        rows = []
        for vector in vectors:
            re, im = split(vector)
            rows.append(
                jnp.concatenate(
                    [jnp.concatenate([re, im], axis=1), jnp.concatenate([-im, re], axis=1)], axis=0
                )
            )
        return jnp.concatenate(rows, axis=0)

    def folded(array):
        return jnp.sum(array.reshape(comps // 8, 8, rhs), axis=0)

    mass = mass_ref[0]
    span = 4 * full

    def matvec(k):
        local = []
        for s in range(sites):
            line, col = s // LX, s % LX
            near = [
                s,
                line * LX + (col + 1) % LX,
                line * LX + (col + LX - 1) % LX,
                (s + LX) % sites,
            ]
            local.append(
                jnp.dot(
                    links_ref[s, :, 0:span], gains([w_buf[k, n] for n in near]),
                    preferred_element_type=F32,
                )
            )
        wait_halo(k)
        sums = None
        for s in range(sites):
            second = gains(
                [w_buf[k, (s + sites - LX) % sites]] + [halo[k, kind, s] for kind in range(3)]
            )
            third = gains([halo[k, 3, s]])
            out = local[s]
            out = out + jnp.dot(links_ref[s, :, span:2 * span], second, preferred_element_type=F32)
            out = out + jnp.dot(links_ref[s, :, 2 * span:], third, preferred_element_type=F32)
            own_re, own_im = split(w_buf[k, s].astype(F32))
            q_re = out[:, :rhs] + mass * own_re
            q_im = out[:, rhs:] + mass * own_im
            q_buf[k, s, 0:comps] = q_re
            q_buf[k, s, comps:full] = q_im
            r_re, r_im = split(r_buf[k, s])
            terms = [
                folded(q_re * q_re + q_im * q_im),
                folded(q_re * r_re + q_im * r_im),
                folded(q_re * r_im - q_im * r_re),
            ]
            for j in range(k):
                e_re, e_im = split(q_buf[j, s])
                terms += [
                    folded(e_re * q_re + e_im * q_im),
                    folded(e_re * q_im - e_im * q_re),
                    folded(e_re * r_re + e_im * r_im),
                    folded(e_re * r_im - e_im * r_re),
                ]
            sums = terms if sums is None else [a + b for a, b in zip(sums, terms)]
        return [jnp.sum(one, axis=0, keepdims=True) for one in sums]

    def all_reduce(k, sums):
        count = len(sums)
        rows = pl.ds(0, count)
        for i, one in enumerate(sums):
            row_send[k, i:i + 1, :] = one
        for d, peer in enumerate(row_peers):
            start(
                remote(row_send.at[k, rows], row_recv.at[k, d, rows], row_ss.at[k, d], row_rs.at[k, d], peer)
            )
        total = row_send[k, 0:count]
        for d in range(len(row_peers)):
            remote(
                row_send.at[k, rows], row_recv.at[k, d, rows], row_ss.at[k, d], row_rs.at[k, d], mate
            ).wait_recv()
            total = total + row_recv[k, d, 0:count]
        col_send[k, 0:count] = total
        for d, peer in enumerate(col_peers):
            start(
                remote(col_send.at[k, rows], col_recv.at[k, d, rows], col_ss.at[k, d], col_rs.at[k, d], peer)
            )
        start(remote(w_buf.at[k], w_home.at[k], home_ss.at[k], home_rs.at[k], to_home))
        for d in range(len(col_peers)):
            remote(
                col_send.at[k, rows], col_recv.at[k, d, rows], col_ss.at[k, d], col_rs.at[k, d], mate
            ).wait_recv()
            total = total + col_recv[k, d, 0:count]
        return [total[i:i + 1] for i in range(count)]

    def minus(value, coefs, basis, s):
        re, im = split(value)
        for j, (c_re, c_im) in enumerate(coefs):
            e_re, e_im = split(basis[j, s])
            re = re - (c_re * e_re - c_im * e_im)
            im = im - (c_re * e_im + c_im * e_re)
        return re, im

    columns = raw.shape[1]
    columns = raw.shape[1]
    own_raw = pltpu.make_async_copy(
        proj_ref.at[pl.ds(pl.multiple_of(y * columns, columns), columns)], raw.at[y], raw_ls
    )
    own_fine = []
    for reim in range(2):
        for h in range(2):
            i = 2 * reim + h
            rows = pl.ds(pl.multiple_of(reim * comps + core * FK, FK), FK)
            own_fine.append(
                pltpu.make_async_copy(
                    fine_ref.at[:, 1 - core, :, reim, h], fine_buf.at[:, :, h, rows], fine_ls.at[i]
                )
            )
    for copy in [own_raw] + own_fine:
        copy.start()

    def links_copy(c):
        span_ = (pl.ds(0, EARLY), pl.ds(EARLY, sites - EARLY))[c]
        return remote(far_links_ref.at[span_], links_ref.at[span_], links_ss.at[c], links_rs.at[c], to_slot)

    met(everyone)
    for dy, peer in enumerate(col_peers):
        rows = pl.ds(pl.multiple_of(rem(y + 1 + dy, YC) * columns, columns), columns)
        start(remote(proj_ref.at[rows], raw.at[y], raw_ss.at[dy], raw_rs.at[dy], peer))
    start(links_copy(0))
    for reim in range(2):
        for h in range(2):
            i = 2 * reim + h
            rows = pl.ds(pl.multiple_of(reim * comps + core * FK, FK), FK)
            start(
                remote(
                    fine_ref.at[:, core, :, reim, h], fine_buf.at[:, :, h, rows], fine_ss.at[i], fine_rs.at[i], mate
                )
            )

    own_raw.wait()
    for dy in range(YC - 1):
        remote(proj_ref.at[pl.ds(0, columns)], raw.at[y], raw_ss.at[dy], raw_rs.at[dy], mate).wait_recv()
    tiles = wide.shape[0]
    for t in range(tiles):
        for yp in range(YC):
            wide[t, 16 * yp:16 * yp + 16] = raw[yp, :, 128 * t:128 * (t + 1)].astype(F32)
    lanes = lax.broadcasted_iota(jnp.int32, (XC * YC, 128), 1)

    def spread_group(group, carry):
        for v in range(8):
            acc = jnp.zeros((XC * YC, 128), F32)
            for c in range(CORES):
                held = {}
                for reim in range(2):
                    first = 2 * FK * v + FK * reim
                    to = 2 * FK * reim + FK * c
                    left = FK
                    while left:
                        tile, off = first // 128, first % 128
                        size = min(left, 128 - off)
                        if tile not in held:
                            held[tile] = wide[3 * group + tile, pl.ds(c, XC * YC, stride=CORES), :]
                        moved = pltpu.roll(held[tile], (to - off) % 128, 1) if to != off else held[tile]
                        acc = jnp.where((lanes >= to) & (lanes < to + size), moved, acc)
                        first, to, left = first + size, to + size, left - size
            spread[pl.ds(8 * group + v, XC * YC, stride=comps), :] = acc
        return carry

    lax.fori_loop(0, comps // 8, spread_group, 0)
    lane = lax.broadcasted_iota(jnp.int32, (8, 128), 1)
    low_lanes = lane < full
    for xc in range(XC):
        for yp in range(YC):
            base = (yp * XC + xc) * comps
            tail = spread[base + PACKED:base + comps]
            head = [
                jnp.where(low_lanes, spread[base + 8 * j:base + 8 * j + 8], pltpu.roll(tail, full - 32 * j, 1))
                for j in range(3)
            ]
            blocks[xc, yp] = jnp.concatenate(head + [spread[base + 24:base + PACKED]], axis=0).astype(BF16)
    owner = 1 - div(x, HALF)
    home_slot = rem(XC - z_home, XC)
    for i, step in enumerate((4, 3, 5, 2, 6, 1, 7, 0)):
        xc = rem(home_slot + step, XC)
        here = jnp.logical_and(xc == x, owner == core)
        copy = remote(blocks.at[xc], packed.at[z_home], blk_ss.at[i], blk_rs.at[z_home], (g, y, xc, owner))

        @pl.when(here)
        def _():
            packed[z_home] = blocks[xc]

        @pl.when(jnp.logical_not(here))
        def _():
            copy.start()

    def product(z, yp):
        lhs = pbuf[z, yp]
        outs = []
        for h in range(2):
            left = fine_buf[yp, z, h]
            right = jnp.concatenate([left[comps:], -left[:comps]], axis=0)
            out = jnp.dot(
                lhs[16 * h:16 * h + 32, :full], jnp.concatenate([left, right], axis=1),
                preferred_element_type=F32,
            )
            outs.append(out[8 * h:8 * h + FK])
        return jnp.concatenate([part_[:, :rhs] for part_ in outs] + [part_[:, rhs:] for part_ in outs], axis=0)

    def wait_blocks(z):
        mine = jnp.logical_and(z == z_home, owner == core)

        @pl.when(jnp.logical_not(mine))
        def _():
            remote(blocks.at[0], packed.at[z], blk_ss.at[0], blk_rs.at[z], mate).wait_recv()

        def unpack(yp, carry):
            held = packed[z, yp]
            rows = held[0:24].astype(F32)
            moved = [pltpu.roll(rows[8 * j:8 * j + 8], 32 * (j + 1), 1) for j in range(3)]
            tail = jnp.where(lane < 32, moved[0], jnp.where(lane < 64, moved[1], moved[2]))
            pbuf[z, yp] = jnp.concatenate([held.astype(F32), tail], axis=0).astype(BF16)
            return carry

        lax.fori_loop(0, YC, unpack, 0)

    for copy in own_fine:
        copy.wait()
    for i in range(4):
        remote(
            fine_ref.at[:, 0, :, 0, 0], fine_buf.at[:, :, 0, pl.ds(0, FK)], fine_ss.at[i], fine_rs.at[i], mate
        ).wait_recv()

    ways = ((1, (g, y, rem(x + 1, XC), core)), (0, (g, y, rem(x + XC - 1, XC), core)))
    waited = set()

    def received(way, m):
        remote(
            chain_send.at[way, m], chain_recv.at[way, m], chain_ss.at[way, m], chain_rs.at[way, m], mate
        ).wait_recv()

    def finish(quarter):
        z = z_slot
        if 0 not in waited:
            waited.add(0)
            wait_blocks(z)
        last = [ORDER[way].index((quarter, 1)) for way in range(2)]
        for way in range(2):
            received(way, last[way])
        for i in range(2):
            yp = 2 * quarter + i
            total_buf[yp] = product(z, yp) + chain_recv[0, last[0], i] + chain_recv[1, last[1], i]

            @pl.when(y == yp)
            def _():
                r_buf[0, yp] = total_buf[yp]

            @pl.when(y != yp)
            def _():
                remote(total_buf.at[yp], r_buf.at[0, y], src_ss.at[yp], src_rs.at[y], (g, yp, x, core)).start()

    for m in range(len(ORDER[0])):
        for way, (plus, peer) in enumerate(ways):
            quarter, d = ORDER[way][m]
            sign = d if plus else -d
            z = rem(XC - rem(x + XC + sign, XC), XC)
            key = sign % XC
            if key not in waited:
                waited.add(key)
                wait_blocks(z)
            before = (quarter, d + 1)
            source = ORDER[way].index(before) if before in ORDER[way] else None
            if source is not None:
                received(way, source)
            for i in range(2):
                value = product(z, 2 * quarter + i)
                if source is not None:
                    value = value + chain_recv[way, source, i]
                chain_send[way, m, i] = value
            start(
                remote(
                    chain_send.at[way, m], chain_recv.at[way, m], chain_ss.at[way, m], chain_rs.at[way, m], peer
                )
            )
        if m in (11, 12):
            finish(m - 11)
    start(links_copy(1))
    finish(2)
    finish(3)
    for dy in (0, 1, 7, 2, 6, 3, 5, 4):
        s = rem(y + dy, YC)
        if dy:
            remote(total_buf.at[s], r_buf.at[0, s], src_ss.at[s], src_rs.at[s], mate).wait_recv()
        w_buf[0, s] = r_buf[0, s].astype(BF16)
        for place, (kind, peer) in enumerate(neighbours):
            start(remote(w_buf.at[0, s], halo.at[0, kind, s], first_ss.at[place, s], first_rs.at[kind, s], peer))
    for c in range(CHUNKS):
        links_copy(c).wait_recv()

    gram = {}
    basis = []
    betas = []
    for k in range(ITERS):
        totals = all_reduce(k, matvec(k))
        squared, a_re, a_im = totals[:3]
        coefs = []
        for j in range(k):
            c_re, c_im, b_re, b_im = totals[3 + 4 * j:7 + 4 * j]
            coefs.append((c_re, c_im))
            a_re = a_re - (c_re * b_re + c_im * b_im)
            a_im = a_im - (c_re * b_im - c_im * b_re)
        for j, (c_re, c_im) in enumerate(coefs):
            squared = squared - (2.0 - gram[j, j][0]) * (c_re * c_re + c_im * c_im)
        for i in range(k):
            for j in range(i + 1, k):
                (u_re, u_im), (v_re, v_im) = coefs[i], coefs[j]
                m_re = u_re * v_re + u_im * v_im
                m_im = u_re * v_im - u_im * v_re
                n_re, n_im = gram[i, j]
                squared = squared + 2.0 * (m_re * n_re - m_im * n_im)
        squared = jnp.maximum(squared, 0.0)
        factor = 1.0 / jnp.sqrt(squared + 1e-06)
        if k + 1 < ITERS:
            gram[k, k] = (squared * factor * factor, None)
            for j, (c_re, c_im) in enumerate(coefs):
                lack_re = (1.0 - gram[j, j][0]) * c_re
                lack_im = (1.0 - gram[j, j][0]) * c_im
                gram[j, k] = (factor * lack_re, factor * lack_im)
        a_re, a_im = a_re * factor, a_im * factor
        last = k + 1 == ITERS
        for c in range(CHUNKS):
            for s in range(c * part, (c + 1) * part):
                q_re, q_im = minus(q_buf[k, s], coefs, q_buf, s)
                q_re, q_im = q_re * factor, q_im * factor
                r_re, r_im = split(r_buf[k, s])
                r_re = r_re - (a_re * q_re - a_im * q_im)
                r_im = r_im - (a_re * q_im + a_im * q_re)
                if last:
                    out_send[s, 0:comps] = r_re.astype(BF16)
                    out_send[s, comps:full] = r_im.astype(BF16)
                else:
                    q_buf[k, s, 0:comps] = q_re
                    q_buf[k, s, comps:full] = q_im
                    r_buf[k + 1, s, 0:comps] = r_re
                    r_buf[k + 1, s, comps:full] = r_im
                    w_buf[k + 1, s, 0:comps] = r_re.astype(BF16)
                    w_buf[k + 1, s, comps:full] = r_im.astype(BF16)
            if last:
                start(
                    remote(out_send.at[chunk(c)], out_recv.at[1, chunk(c)], out_ss.at[c], out_rs.at[c], to_home)
                )
            else:
                send_halo(k + 1, c)
        row = [(0.0, 0.0)] * k + [(factor, 0.0)]
        for j, (c_re, c_im) in enumerate(coefs):
            f_re, f_im = factor * c_re, factor * c_im
            for i in range(j + 1):
                u_re, u_im = basis[j][i]
                row[i] = (row[i][0] - (f_re * u_re - f_im * u_im), row[i][1] - (f_re * u_im + f_im * u_re))
        basis.append(row)
        for i in range(k + 1):
            u_re, u_im = row[i]
            b_re, b_im = betas[i] if i < len(betas) else (0.0, 0.0)
            term = (b_re + a_re * u_re - a_im * u_im, b_im + a_re * u_im + a_im * u_re)
            betas[i:i + 1] = [term]
    for k in range(ITERS):
        remote(w_buf.at[k], w_home.at[k], home_ss.at[k], home_rs.at[k], mate).wait_recv()
    for s in range(sites):
        s_re = s_im = 0.0
        for k in range(ITERS):
            b_re, b_im = betas[k]
            e_re, e_im = split(w_home[k, s].astype(F32))
            s_re = s_re + (b_re * e_re - b_im * e_im)
            s_im = s_im + (b_re * e_im + b_im * e_re)
        out_recv[0, s, 0:comps] = s_re.astype(BF16)
        out_recv[0, s, comps:full] = s_im.astype(BF16)
    for c in range(CHUNKS):
        remote(out_send.at[chunk(c)], out_recv.at[1, chunk(c)], out_ss.at[c], out_rs.at[c], mate).wait_recv()
    for copy in pending:
        copy.wait_send()
    for i, step in enumerate((4, 3, 5, 2, 6, 1, 7, 0)):
        xc = rem(home_slot + step, XC)

        @pl.when(jnp.logical_not(jnp.logical_and(xc == x, owner == core)))
        def _():
            remote(blocks.at[xc], packed.at[z_home], blk_ss.at[i], blk_rs.at[z_home], mate).wait_send()

    for yp in range(YC):

        @pl.when(y != yp)
        def _():
            remote(total_buf.at[yp], r_buf.at[0, yp], src_ss.at[yp], src_rs.at[yp], mate).wait_send()


def shards(fine_source, projectors, stencil_links, quark_mass):
    sites, comps, width = stencil_links.shape[1:]
    rhs = fine_source.shape[-1]
    full = 2 * comps
    columns, row = projectors.shape[1:]
    fine = fine_source.reshape(YC, 2, XC, 2, 2, FK, rhs)
    vector = (sites, full, rhs)
    most = 3 + 4 * (ITERS - 1)
    rows = -(-most // 8) * 8
    peers_x, peers_y = XC * CORES - 1, YC - 1
    dma = pltpu.SemaphoreType.DMA
    vmem = pl.BlockSpec(memory_space=pltpu.VMEM)
    hbm = pl.BlockSpec(memory_space=pltpu.HBM)
    messages = len(ORDER[0])
    result = pl.pallas_call(
        solve_kernel,
        out_shape=jax.ShapeDtypeStruct((2,) + vector, BF16),
        in_specs=[pl.BlockSpec(memory_space=pltpu.SMEM), hbm, hbm, hbm],
        out_specs=vmem,
        scratch_shapes=[
            pltpu.VMEM((YC, XC, 2, full, rhs), BF16),
            pltpu.VMEM((YC, columns // YC, row), BF16),
            pltpu.VMEM((row // 128, columns, 128), F32),
            pltpu.VMEM((XC * YC * comps, 128), F32),
            pltpu.VMEM((XC, YC, PACKED, 128), BF16),
            pltpu.VMEM((XC, YC, PACKED, 128), BF16),
            pltpu.VMEM((XC, YC, comps, 128), BF16),
            pltpu.VMEM((2, messages, 2, full, rhs), F32),
            pltpu.VMEM((2, messages, 2, full, rhs), F32),
            pltpu.VMEM((YC, full, rhs), F32),
            pltpu.VMEM((sites, comps, width), BF16),
            pltpu.VMEM((ITERS,) + vector, F32),
            pltpu.VMEM((ITERS,) + vector, BF16),
            pltpu.VMEM((ITERS, 4) + vector, BF16),
            pltpu.VMEM((ITERS,) + vector, F32),
            pltpu.VMEM((ITERS,) + vector, BF16),
            pltpu.VMEM((ITERS, rows, rhs), F32),
            pltpu.VMEM((ITERS, peers_x, rows, rhs), F32),
            pltpu.VMEM((ITERS, rows, rhs), F32),
            pltpu.VMEM((ITERS, peers_y, rows, rhs), F32),
            pltpu.VMEM(vector, BF16),
            dma((CHUNKS,)), dma((CHUNKS,)), dma((4,)), dma((4,)), dma((4,)),
            dma(()), dma((peers_y,)), dma((peers_y,)),
            dma((XC,)), dma((XC,)),
            dma((2, messages)), dma((2, messages)),
            dma((YC,)), dma((YC,)),
            dma((4, sites)), dma((4, sites)),
            dma((ITERS, 4, CHUNKS)), dma((ITERS, 4, CHUNKS)),
            dma((ITERS, peers_x)), dma((ITERS, peers_x)),
            dma((ITERS, peers_y)), dma((ITERS, peers_y)),
            dma((ITERS,)), dma((ITERS,)), dma((CHUNKS,)), dma((CHUNKS,)),
        ],
        compiler_params=pltpu.CompilerParams(
            collective_id=0, has_side_effects=True, vmem_limit_bytes=56 * 1024 * 1024
        ),
        name="restrict_and_solve",
    )(quark_mass, fine, projectors[0], stencil_links[0])
    result = result.astype(F32)
    return result[0:1], result[1:2]


def solution(mesh):
    finer = Mesh(mesh.devices.reshape(mesh.shape["cfg"], YC, XC, CORES), ALL)
    placed = (
        P("cfg", GROUP, None, None, None, None),
        P(ALL, None, None),
        P(ALL, None, None, None),
        P("cfg"),
    )
    return jax.shard_map(
        shards,
        mesh=finer,
        in_specs=placed,
        out_specs=(P(ALL, None, None, None), P(ALL, None, None, None)),
        check_vma=False,
    )
```
